32 devices in a mesh: comp: 8 (over z, core), blk: 4 (over y, x).
Axes of the slice: x: 2, y: 2, z: 4, core: 2. Of those that a mesh axis runs over, the one named last changes fastest.
Arguments:
- state_now: float32 [8, 6, 32, 32, 256], P('comp', None, 'blk'), may hold values from -5 to 5
- state_prev: float32 [8, 6, 32, 32, 256], P('comp', None, 'blk'), may hold values from -5 to 5
- viscosity: float32 [8, 32, 32, 256], P('comp', 'blk'), may hold values from 0.05 to 0.5
- jacobian: float32 [8, 3, 6, 6], P('comp'), may hold values from -0.4 to 0.4
- donor_cell: int32 [8, 4, 8, 2, 8, 128], P('comp', 'blk'), may hold values from 0 to 57343, as said below
- interp_weight: float32 [8, 4, 8, 2, 8, 128], P('comp', 'blk'), may hold values from 0 to 1
- recv_cell: int32 [8, 4, 8, 2, 128], P('comp', 'blk'), may hold values from 0 to 57343, as said below
- pair_tiles: int32 [4, 8, 8], P('blk'), may hold values from 0 to 2, as said below
Outputs:
- state_next: float32 [8, 6, 32, 32, 256], P('comp', None, 'blk')
The draws below stay inside these ranges and needn't reach their ends.
Inputs may be any that keep to these rules, and one draw needn't show every extreme that they name: `donor_cell`: the cells of one donor tile point are the eight corners of a cube of adjacent cells, corner k = 4 i + 2 j + l offset by (i, j, l). `recv_cell`: the receiving cells of one device are all different. `pair_tiles`: for each block index some destination component takes 2 tiles from every source component.
All inputs are finite; a program needn't handle non-finite values.
Results may differ from the reference program's by a relative error of at most 0.0003.
Values sent between devices are 32-bit elements; how exact they have to be, the bound alone decides.
A program may use at most 128 MiB of HBM per device.

```python
import math
import jax
import jax.numpy as jnp
from jax import lax

NV = 6
CX = 8
CY = 32
CZ = 256
SLOT = 2
TILE = 128
SUBITERS = 2
COMPS = 8
BLKS = 4
NX = 32
CELLS = 65536


def draw_donor_cell(key, part):
    shape = (COMPS, BLKS, COMPS, SLOT, TILE)
    first = jax.random.randint(jax.random.fold_in(key, 11), shape, 0, CX - 2)
    second = jax.random.randint(jax.random.fold_in(key, 12), shape, 0, CY - 1)
    third = jax.random.randint(jax.random.fold_in(key, 13), shape, 0, CZ - 1)
    corners = []
    for corner in range(8):
        off_a = corner // 4
        off_b = corner // 2 % 2
        off_c = corner % 2
        corners.append(((first + off_a) * CY + (second + off_b)) * CZ + (third + off_c))
    return jnp.stack(corners, axis=4).astype(jnp.int32)


def draw_interp_weight(key, part):
    shape = (3, COMPS, BLKS, COMPS, SLOT, TILE)
    frac = jax.random.uniform(jax.random.fold_in(key, 22), shape, jnp.float32)
    corners = []
    for corner in range(8):
        off_a = corner // 4
        off_b = corner // 2 % 2
        off_c = corner % 2
        part_a = frac[0] if off_a == 1 else 1.0 - frac[0]
        part_b = frac[1] if off_b == 1 else 1.0 - frac[1]
        part_c = frac[2] if off_c == 1 else 1.0 - frac[2]
        corners.append(part_a * part_b * part_c)
    return jnp.stack(corners, axis=4).astype(jnp.float32)


def draw_recv_cell(key, part):
    keys = jax.random.split(jax.random.fold_in(key, 31), COMPS * BLKS)

    def one_device(single):
        return jax.random.permutation(single, (CX - 1) * CY * CZ)[:COMPS * SLOT * TILE]
    chosen = jax.vmap(one_device)(keys)
    return chosen.reshape(COMPS, BLKS, COMPS, SLOT, TILE).astype(jnp.int32)


def draw_pair_tiles(key, part):
    counts = jax.random.randint(jax.random.fold_in(key, 41), (BLKS, COMPS, COMPS), 0, SLOT + 1)
    column = jax.random.randint(jax.random.fold_in(key, 42), (BLKS,), 0, COMPS)
    full = jnp.arange(COMPS, dtype=jnp.int32)[None, None, :] == column[:, None, None]
    return jnp.where(full, SLOT, counts).astype(jnp.int32)


def block_scale(own_key, extent, cuts, smallest, high):
    gain = 1.0
    for axis_at, shards_of in cuts:
        heights = jax.random.uniform(jax.random.fold_in(jax.random.fold_in(own_key, 6), axis_at), (shards_of,), jnp.float32, smallest / len(cuts), high / len(cuts))
        gain = gain * jnp.repeat(jnp.exp(heights), extent[axis_at] // shards_of).reshape((-1,) + (1,) * (len(extent) - 1 - axis_at))
    return gain


def bell_draw(own_key, shape, deviation, limit, pieces=(), held_as=jnp.bfloat16):
    factor_of = block_scale(own_key, shape, pieces, -0.22, 0.18) if pieces else 1.0
    drawn = jax.random.normal(own_key, shape, jnp.float32) * deviation * factor_of
    return jnp.minimum(jnp.maximum(drawn, -limit), limit).astype(held_as)


def setup_inputs(seed: int = 0) -> dict:
    streams_of = jax.random.split(jax.random.key(seed), 9)
    return {
        "state_now": bell_draw(streams_of[0], (COMPS, NV, NX, CY, CZ), 1.0, 5.0, ((0, 8), (2, 4)), jnp.float32),
        "state_prev": bell_draw(streams_of[1], (COMPS, NV, NX, CY, CZ), 1.0, 5.0, ((0, 8), (2, 4)), jnp.float32),
        "viscosity": jnp.clip(jnp.exp(math.log(0.5) - 2.3025851 * jax.random.uniform(streams_of[2], (COMPS, NX, CY, CZ), jnp.float32) ** block_scale(streams_of[2], (COMPS, NX, CY, CZ), ((0, 8), (1, 4)), -0.2, 0.2)), 0.05, 0.5),
        "jacobian": bell_draw(streams_of[3], (COMPS, 3, NV, NV), 0.1, 0.4, ((0, 8),), jnp.float32),
        "donor_cell": draw_donor_cell(jax.random.fold_in(streams_of[8], 71), 0),
        "interp_weight": draw_interp_weight(jax.random.fold_in(streams_of[8], 71), 0),
        "recv_cell": draw_recv_cell(jax.random.fold_in(streams_of[8], 71), 0),
        "pair_tiles": draw_pair_tiles(jax.random.fold_in(streams_of[8], 71), 0),
    }


time_scale = 0.5
pseudo_diag = 2.5


def mix(jac_dim, field):
    return jnp.einsum('vw,wxyz->vxyz', jac_dim, field, precision=lax.Precision.HIGHEST)


def flux(padded, kappa, jac):
    centre = padded[:, 1:-1]
    along_x = (padded[:, 2:] - padded[:, :-2]) * 0.5
    spread = jnp.pad(centre, ((0, 0), (0, 0), (1, 1), (1, 1)))
    along_y = (spread[:, :, 2:, 1:-1] - spread[:, :, :-2, 1:-1]) * 0.5
    along_z = (spread[:, :, 1:-1, 2:] - spread[:, :, 1:-1, :-2]) * 0.5
    beside = padded[:, 2:] + padded[:, :-2] + spread[:, :, 2:, 1:-1] + spread[:, :, :-2, 1:-1]
    beside = beside + spread[:, :, 1:-1, 2:] + spread[:, :, 1:-1, :-2]
    convect = mix(jac[0], along_x) + mix(jac[1], along_y) + mix(jac[2], along_z)
    return convect + kappa * (6.0 * centre - beside)


def relax(rstar, padded_step, kappa, diag, jac):
    centre = padded_step[:, 1:-1]
    return -(rstar + flux(padded_step, kappa, jac) - 6.0 * kappa * centre) / diag


def pad_rows(field):
    return jnp.pad(field, ((0, 0), (1, 1), (0, 0), (0, 0)))


def subiteration(items):
    state, now, prev, kappa, jac = items
    diag = pseudo_diag + 6.0 * kappa
    rstar = time_scale * (3.0 * state - 4.0 * now + prev) + flux(pad_rows(state), kappa, jac)
    first = -rstar / diag
    second = relax(rstar, pad_rows(first), kappa, diag, jac)
    third = relax(rstar, pad_rows(second), kappa, diag, jac)
    return state + third


def fringe(state, donor_cell, interp_weight, recv_cell, pair_tiles):
    comps = state.shape[0]
    nvar = state.shape[1]
    flat = state.reshape(comps, nvar, BLKS, CELLS).transpose(2, 0, 1, 3)
    donors = donor_cell.transpose(1, 0, 2, 3, 4, 5)
    weights = interp_weight.transpose(1, 0, 2, 3, 4, 5)
    cells_all = recv_cell.transpose(1, 0, 2, 3, 4)

    def one_block(items):
        blocks, donor_b, weight_b, cell_b, live_b = items

        def pick(block, index):
            return block[:, index.reshape(-1)]

        values = jax.vmap(pick)(blocks, donor_b).reshape(comps, nvar, comps, SLOT, 8, TILE)
        interp = jnp.einsum('caskp,avcskp->cvasp', weight_b, values, precision=lax.Precision.HIGHEST)

        def place(block, cells, incoming, live):
            index = cells.reshape(-1)
            keep = jnp.arange(SLOT, dtype=jnp.int32)[None, :] < live[:, None]
            keep = jnp.broadcast_to(keep[:, :, None], (comps, SLOT, TILE)).reshape(-1)
            old = block[:, index]
            return block.at[:, index].set(jnp.where(keep[None, :], incoming.reshape(nvar, -1), old))

        return jax.vmap(place)(blocks, cell_b, interp, live_b.T)

    result = lax.map(one_block, (flat, donors, weights, cells_all, pair_tiles))
    return result.transpose(1, 2, 0, 3).reshape(state.shape)


def reference(state_now, state_prev, viscosity, jacobian, donor_cell, interp_weight, recv_cell, pair_tiles):
    state = state_now
    for sub in range(SUBITERS):
        state = lax.map(subiteration, (state, state_now, state_prev, viscosity, jacobian))
        state = fringe(state, donor_cell, interp_weight, recv_cell, pair_tiles)
    return state
```

```python
import functools

import jax
import jax.numpy as jnp
from jax import lax
from jax.experimental import pallas as pl
from jax.experimental.pallas import tpu as pltpu
from jax.sharding import PartitionSpec as P

SUBITERS = 2


time_scale = 0.5
pseudo_diag = 2.5

MESH = pl.DeviceIdType.MESH
VMEM_LIMIT = 60 * 1024 * 1024
F32 = jnp.float32
BF16 = jnp.bfloat16
I32 = jnp.int32
LANES = 128
SUB = 8
PAD = SUB


def split(value):
    high = value.astype(BF16)
    low = (value - high.astype(F32)).astype(BF16)
    return high, low


def flux_tile(src, coef, x, y, kappa, centred):
    nvar, _, halves, _, _ = src.shape
    lane = lax.broadcasted_iota(I32, (SUB, LANES), 1)
    total = [[None] * halves for _ in range(nvar)]
    for w in range(nvar):
        centre = [src[w, x + 1, h, pl.ds(PAD + y, SUB), :] for h in range(halves)]
        fore = [pltpu.roll(c, LANES - 1, 1) for c in centre]
        back = [pltpu.roll(c, 1, 1) for c in centre]
        for h in range(halves):
            next_z = jnp.where(lane == LANES - 1, fore[h + 1] if h + 1 < halves else 0.0, fore[h])
            last_z = jnp.where(lane == 0, back[h - 1] if h > 0 else 0.0, back[h])
            next_x = src[w, x + 2, h, pl.ds(PAD + y, SUB), :]
            last_x = src[w, x, h, pl.ds(PAD + y, SUB), :]
            next_y = src[w, x + 1, h, pl.ds(PAD + y + 1, SUB), :]
            last_y = src[w, x + 1, h, pl.ds(PAD + y - 1, SUB), :]
            beside = (next_x + last_x) + (next_y + last_y) + (next_z + last_z)
            if centred:
                own = kappa[h] * (6.0 * centre[h] - beside)
            else:
                own = -kappa[h] * beside
            total[w][h] = own if total[w][h] is None else total[w][h] + own
            diffs = (next_x - last_x, next_y - last_y, next_z - last_z)
            for v in range(nvar):
                term = None
                for d in range(3):
                    part = coef[(d * nvar + v) * nvar + w] * diffs[d]
                    term = part if term is None else term + part
                total[v][h] = term if total[v][h] is None else total[v][h] + term
    return total


def fill_hots(cells, row_hot, z_hot, shift):
    tiles, tile = cells.shape
    pairs = row_hot.shape[0]
    width_z = z_hot.shape[0]

    def one(t, carry):
        cell = cells[pl.ds(t, 1), :]
        pair = lax.shift_right_arithmetic(cell, shift)
        depth = jnp.bitwise_and(cell, width_z - 1)
        at = pl.ds(pl.multiple_of(t * tile, tile), tile)
        here = lax.broadcasted_iota(I32, (pairs, tile), 0) == pair
        row_hot[:, at] = jnp.where(here, 1.0, 0.0).astype(BF16)
        deep = lax.broadcasted_iota(I32, (width_z, tile), 0) == depth
        z_hot[:, at] = jnp.where(deep, 1.0, 0.0).astype(BF16)
        return carry

    lax.fori_loop(0, tiles, one, 0)


def fill_values(values, spread):
    comps, slots, nvar, tile = values.shape
    depth = spread.shape[1]

    def one(t, carry):
        high, low = split(values[lax.div(t, slots), lax.rem(t, slots)])
        at = pl.ds(pl.multiple_of(t * tile, tile), tile)
        for v in range(nvar):
            spread[v, :, at] = jnp.broadcast_to(high[v : v + 1].astype(F32), (depth, tile)).astype(BF16)
            spread[nvar + v, :, at] = jnp.broadcast_to(low[v : v + 1].astype(F32), (depth, tile)).astype(BF16)
        return carry

    lax.fori_loop(0, comps * slots, one, 0)


def place_plane(x, row_hot, z_hot, spread, placed):
    parts, depth, points = spread.shape
    width_y = placed.shape[0] // (parts + 1)

    def one(t, carry):
        at = pl.ds(pl.multiple_of(t * LANES, LANES), LANES)
        rows = row_hot[pl.ds(pl.multiple_of(x * width_y, width_y), width_y), at]
        for j in range(parts):
            value = jnp.concatenate([spread[j, :, at]] * (width_y // depth), axis=0)
            placed[j * width_y : (j + 1) * width_y, at] = rows * value
        placed[parts * width_y :, at] = rows
        return carry

    lax.fori_loop(0, points // LANES, one, 0)
    return lax.dot_general(placed[...], z_hot[...], (((1,), (1,)), ((), ())), preferred_element_type=F32)


def main_kernel(
    count, comps, jac_ref, live_ref, now_ref, prev_ref, kappa_ref, donor_ref, weight_ref, recv_ref,
    out_ref, arrived, cells,
    state, first, second, rstar, hist, kappa, scale, coef,
    packed, values, held, weight_land, landing, row_hot, z_hot, spread, placed,
    load_sem, halo_send, halo_recv, weight_send, weight_recv, value_send, value_recv, save_sem,
):
    me = lax.axis_index("blk")
    mine = lax.axis_index("comp")
    right = lax.rem(me + 1, count)
    left = lax.rem(me + count - 1, count)
    has_left = me > 0
    has_right = me < count - 1
    nvar, rows, halves, width_y, _ = rstar.shape
    width_z = halves * LANES
    shift = width_z.bit_length() - 1
    chunks = width_y // SUB
    slots, corners, tile = donor_ref.shape[1:]
    fields = [state, first, second]
    inside = pl.ds(PAD, width_y)
    edge = rows - 1

    def lanes(h):
        return pl.ds(h * LANES, LANES)

    loads = []
    for h in range(halves):
        for x in (0, edge):
            loads.append((now_ref.at[:, x, :, lanes(h)], state.at[:, x + 1, h, inside, :]))
    for h in range(halves):
        loads.append((now_ref.at[:, pl.ds(1, rows - 2), :, lanes(h)], state.at[:, pl.ds(2, rows - 2), h, inside, :]))
    for h in range(halves):
        loads.append((kappa_ref.at[:, :, lanes(h)], kappa.at[:, h]))
    for h in range(halves):
        loads.append((prev_ref.at[:, :, :, lanes(h)], hist.at[:, :, h]))
    loads = [pltpu.make_async_copy(src, dst, load_sem.at[i]) for i, (src, dst) in enumerate(loads)]
    for load in loads:
        load.start()

    barrier = pltpu.get_barrier_semaphore()

    @pl.when(has_left)
    def _():
        pl.semaphore_signal(barrier, inc=1, device_id={"blk": left}, device_id_type=MESH)

    @pl.when(has_right)
    def _():
        pl.semaphore_signal(barrier, inc=1, device_id={"blk": right}, device_id_type=MESH)

    for d in range(1, comps):
        peer = lax.rem(mine + d, comps)
        pl.semaphore_signal(barrier, inc=1, device_id={"comp": peer}, device_id_type=MESH)

    def blank_pads(x, carry):
        for field in fields:
            for v in range(nvar):
                for h in range(halves):
                    field[v, x + 1, h, 0:PAD, :] = jnp.zeros((PAD, LANES), F32)
                    field[v, x + 1, h, PAD + width_y :, :] = jnp.zeros((field.shape[3] - PAD - width_y, LANES), F32)
        return carry

    lax.fori_loop(0, rows, blank_pads, 0)

    def blank_plane(x):
        for field in fields:
            for v in range(nvar):
                for h in range(halves):
                    field[v, x, h, PAD : PAD + width_y, :] = jnp.zeros((width_y, LANES), F32)

    @pl.when(jnp.logical_not(has_left))
    def _():
        blank_plane(0)

    @pl.when(jnp.logical_not(has_right))
    def _():
        blank_plane(rows + 1)

    def to_left(sub, k, c):
        at = pl.ds(PAD + c * SUB, SUB)
        return pltpu.make_async_remote_copy(
            src_ref=fields[k].at[:, 1, :, at, :], dst_ref=fields[k].at[:, rows + 1, :, at, :],
            send_sem=halo_send.at[sub, k, 1, c], recv_sem=halo_recv.at[sub, k, 1, c],
            device_id={"blk": left}, device_id_type=MESH,
        )

    def to_right(sub, k, c):
        at = pl.ds(PAD + c * SUB, SUB)
        return pltpu.make_async_remote_copy(
            src_ref=fields[k].at[:, rows, :, at, :], dst_ref=fields[k].at[:, 0, :, at, :],
            send_sem=halo_send.at[sub, k, 0, c], recv_sem=halo_recv.at[sub, k, 0, c],
            device_id={"blk": right}, device_id_type=MESH,
        )

    def start(sub, k, c):
        @pl.when(has_left)
        def _():
            to_left(sub, k, c).start()

        @pl.when(has_right)
        def _():
            to_right(sub, k, c).start()

    def arrive(sub, k, c):
        @pl.when(has_left)
        def _():
            to_right(sub, k, c).wait_recv()

        @pl.when(has_right)
        def _():
            to_left(sub, k, c).wait_recv()

    def sent(sub, k):
        for c in range(chunks):
            @pl.when(has_left)
            def _(c=c):
                to_left(sub, k, c).wait_send()

            @pl.when(has_right)
            def _(c=c):
                to_right(sub, k, c).wait_send()

    def comp_copy(d, source, target, send_sem, recv_sem):
        peer = lax.rem(mine + d, comps)
        return pltpu.make_async_remote_copy(
            src_ref=source.at[peer], dst_ref=target.at[d], send_sem=send_sem, recv_sem=recv_sem,
            device_id={"comp": peer}, device_id_type=MESH,
        )

    def weight_copy(d):
        return comp_copy(d, weight_ref, weight_land, weight_send.at[d], weight_recv.at[d])

    def value_copy(sub, d):
        return comp_copy(d, values.at[sub], landing.at[sub], value_send.at[sub, d], value_recv.at[sub, d])

    def tile_step(k, x, c):
        y = c * SUB
        at = pl.ds(y, SUB)
        own = [kappa[x, h, at, :] for h in range(halves)]
        flow = flux_tile(fields[k], coef, x, y, own, k == 0)
        for h in range(halves):
            factor = scale[x, h, at, :]
            for v in range(nvar):
                centre = fields[0][v, x + 1, h, pl.ds(PAD + y, SUB), :]
                if k == 0:
                    base = (3.0 * time_scale) * centre + hist[v, x, h, at, :] + flow[v][h]
                    rstar[v, x, h, at, :] = base
                    first[v, x + 1, h, pl.ds(PAD + y, SUB), :] = base * factor
                else:
                    step = (rstar[v, x, h, at, :] + flow[v][h]) * factor
                    if k == 1:
                        second[v, x + 1, h, pl.ds(PAD + y, SUB), :] = step
                    else:
                        state[v, x + 1, h, pl.ds(PAD + y, SUB), :] = centre + step

    def planes(k, low, high):
        def one(x, carry):
            for c in range(chunks):
                tile_step(k, x, c)
            return carry

        lax.fori_loop(low, high, one, 0)

    def edges(k, c):
        def one(i, carry):
            tile_step(k, i * edge, c)
            return carry

        lax.fori_loop(0, 2, one, 0)

    def pack(low, high, stride, place):
        def one(i, carry):
            x = low + i * stride
            for v in range(nvar):
                at = pl.ds(pl.multiple_of(((place + i) * nvar + v) * width_y, width_y), width_y)
                for h in range(halves):
                    upper, lower = split(state[v, x + 1, h, inside, :])
                    packed[at, h * LANES : (h + 1) * LANES] = upper
                    packed[at, width_z + h * LANES : width_z + (h + 1) * LANES] = lower
            return carry

        lax.fori_loop(0, high, one, 0)

    def interpolate(target, c, s, where, place):
        base = donor_ref[c, s, 0:1, :]
        weights = held[c, s]
        pair = lax.shift_right_logical(base, shift)
        depth = jnp.bitwise_and(base, width_z - 1)
        depth = jnp.concatenate([depth, depth + 1], axis=1)
        pair = jnp.concatenate([pair, pair], axis=1)
        at_z = lax.broadcasted_iota(I32, (width_z, 2 * tile), 0)
        hot = jnp.where(at_z == depth, 1.0, 0.0).astype(BF16)
        hot = jnp.concatenate([hot, hot], axis=0)
        size = nvar * width_y
        found = jnp.dot(packed[place * size : (place + len(where)) * size, :], hot, preferred_element_type=F32)
        total = None
        for i, x in enumerate(where):
            at_pair = lax.broadcasted_iota(I32, (width_y, 2 * tile), 0) + x * width_y - pair
            spread_row = jnp.zeros((width_y, 2 * tile), F32)
            for a in range(2):
                for b in range(2):
                    k = 4 * a + 2 * b
                    row = jnp.concatenate([weights[k : k + 1], weights[k + 1 : k + 2]], axis=1)
                    spread_row = jnp.where(at_pair == a * width_y + b, row, spread_row)
            part = found[i * size : (i + 1) * size].reshape(nvar, width_y, 2 * tile) * spread_row[None]
            total = part if total is None else total + part
        total = total.sum(axis=1)
        return total[:, :tile] + total[:, tile:]

    for load in loads[: 2 * halves]:
        load.wait()
    blocks = has_left.astype(I32) + has_right.astype(I32)
    pl.semaphore_wait(barrier, blocks + comps - 1)
    for c in range(chunks):
        start(0, 0, c)
    for d in range(1, comps):
        weight_copy(d).start()
    for d in range(3):
        for v in range(nvar):
            for w in range(nvar):
                coef[(d * nvar + v) * nvar + w] = jnp.full((SUB, LANES), 0.5 * jac_ref[d, v, w], F32)
    for load in loads[2 * halves :]:
        load.wait()

    def prepare(x, carry):
        scale[x] = -1.0 / (pseudo_diag + 6.0 * kappa[x])
        for v in range(nvar):
            hist[v, x] = time_scale * hist[v, x] - (4.0 * time_scale) * state[v, x + 1, :, inside, :]
        return carry

    lax.fori_loop(0, rows, prepare, 0)

    for sub in range(SUBITERS):
        planes(0, 1, edge)
        if sub == 0:
            for c in range(comps):
                alive = live_ref[c, mine]
                slot = lax.broadcasted_iota(I32, (slots, tile), 0)
                cells[c * slots : (c + 1) * slots, :] = jnp.where(slot < alive, recv_ref[c], -1)
            fill_hots(cells, row_hot, z_hot, shift)
        for c in range(chunks):
            arrive(sub, 0, c)
            edges(0, c)
            start(sub, 1, c)
        low = 1
        for c in range(chunks):
            arrive(sub, 1, c)
            edges(1, c)
            start(sub, 2, c)
            high = low + (edge - low + chunks - c - 1) // (chunks - c)
            planes(1, low, high)
            low = high
        if sub == 0:
            for d in range(1, comps):
                weight_copy(d).wait()
                held[lax.rem(mine - d + comps, comps)] = weight_land[d]
            held[mine] = weight_ref[mine]
        planes(2, 1, edge)
        pack(1, rows - 2, 1, 0)

        def interior(c, carry, sub=sub):
            for s in range(slots):
                values[sub, c, s] = interpolate(sub, c, s, tuple(range(1, edge)), 0)
            return carry

        lax.fori_loop(0, comps, interior, 0)
        sent(sub, 0)
        for c in range(chunks):
            arrive(sub, 2, c)
            edges(2, c)
        pack(0, 2, edge, rows - 2)

        def boundary(d, carry, sub=sub):
            peer = lax.rem(mine + d, comps)
            for s in range(slots):
                values[sub, peer, s] += interpolate(sub, peer, s, (0, edge), rows - 2)

            @pl.when(d > 1)
            def _():
                value_copy(sub, d - 1).start()

            return carry

        lax.fori_loop(1, comps + 1, boundary, 0)
        if sub == SUBITERS - 1:
            saves = [
                pltpu.make_async_copy(
                    state.at[:, pl.ds(1, rows), h, inside, :], out_ref.at[:, :, :, lanes(h)], save_sem.at[h]
                )
                for h in range(halves)
            ]
            for save in saves:
                save.start()
        sent(sub, 1)
        sent(sub, 2)
        arrived[mine] = values[sub, mine]

        def collect(d, carry, sub=sub):
            value_copy(sub, d).wait_recv()
            arrived[lax.rem(mine - d + comps, comps)] = landing[sub, d]
            return carry

        lax.fori_loop(1, comps, collect, 0)
        if sub < SUBITERS - 1:
            fill_values(arrived, spread)

            def place(x):
                part = place_plane(x, row_hot, z_hot, spread, placed)
                hit = part[2 * nvar * width_y :, :] > 0.5
                for v in range(nvar):
                    value = part[v * width_y : (v + 1) * width_y] + part[(nvar + v) * width_y : (nvar + v + 1) * width_y]
                    for h in range(halves):
                        side = slice(h * LANES, (h + 1) * LANES)
                        old = state[v, x + 1, h, inside, :]
                        state[v, x + 1, h, inside, :] = jnp.where(hit[:, side], value[:, side], old)

            def outer(i, carry):
                place(i * edge)
                return carry

            lax.fori_loop(0, 2, outer, 0)
            for c in range(chunks):
                start(sub + 1, 0, c)

            def inner(x, carry):
                place(x)
                return carry

            lax.fori_loop(1, edge, inner, 0)
    for sub in range(SUBITERS):
        for d in range(1, comps):
            value_copy(sub, d).wait_send()
    for save in saves:
        save.wait()


def run_main(jac, live, now, prev, kappa, donor, weights, recv):
    count = lax.axis_size("blk")
    nvar, rows, width_y, width_z = now.shape
    comps, slots, corners, tile = weights.shape
    halves = width_z // LANES
    chunks = width_y // SUB
    points = comps * slots * tile
    pairs = rows * width_y
    vmem = pl.BlockSpec(memory_space=pltpu.VMEM)
    smem = pl.BlockSpec(memory_space=pltpu.SMEM)
    hbm = pl.BlockSpec(memory_space=pl.ANY)
    field = pltpu.VMEM((nvar, rows + 2, halves, width_y + 2 * PAD, LANES), F32)
    plain = pltpu.VMEM((nvar, rows, halves, width_y, LANES), F32)
    single = pltpu.VMEM((rows, halves, width_y, LANES), F32)
    dma = pltpu.SemaphoreType.DMA
    fringe = (comps, slots, nvar, tile)
    scratch = [
        field, field, field, plain, plain, single, single,
        pltpu.VMEM((3 * nvar * nvar, SUB, LANES), F32),
        pltpu.VMEM((nvar * pairs, 2 * width_z), BF16),
        pltpu.VMEM((SUBITERS,) + fringe, F32),
        pltpu.VMEM(weights.shape, F32),
        pltpu.VMEM(weights.shape, F32),
        pltpu.VMEM((SUBITERS,) + fringe, F32),
        pltpu.VMEM((pairs, points), BF16),
        pltpu.VMEM((width_z, points), BF16),
        pltpu.VMEM((2 * nvar, 2 * SUB, points), BF16),
        pltpu.VMEM(((2 * nvar + 1) * width_y, points), BF16),
        dma((6 * halves,)),
        dma((SUBITERS, 3, 2, chunks)), dma((SUBITERS, 3, 2, chunks)),
        dma((comps,)), dma((comps,)),
        dma((SUBITERS, comps)), dma((SUBITERS, comps)),
        dma((halves,)),
    ]
    return pl.pallas_call(
        functools.partial(main_kernel, count, comps),
        out_shape=[
            jax.ShapeDtypeStruct(now.shape, F32),
            jax.ShapeDtypeStruct(fringe, F32),
            jax.ShapeDtypeStruct((comps * slots, tile), I32),
        ],
        in_specs=[smem, smem, hbm, hbm, hbm, vmem, vmem, vmem],
        out_specs=[hbm, vmem, vmem],
        scratch_shapes=scratch,
        compiler_params=pltpu.CompilerParams(
            collective_id=0, has_side_effects=True, vmem_limit_bytes=VMEM_LIMIT
        ),
        name="subiterate",
    )(jac, live, now, prev, kappa, donor, weights, recv)


def finish_kernel(shift, state_ref, cells_ref, value_ref, out_ref, row_hot, z_hot, spread, placed):
    nvar, _, width_y, width_z = state_ref.shape
    x = pl.program_id(0)

    @pl.when(x == 0)
    def _():
        fill_hots(cells_ref, row_hot, z_hot, shift)
        fill_values(value_ref, spread)

    part = place_plane(x, row_hot, z_hot, spread, placed)
    hit = part[2 * nvar * width_y :, :] > 0.5
    for v in range(nvar):
        value = part[v * width_y : (v + 1) * width_y] + part[(nvar + v) * width_y : (nvar + v + 1) * width_y]
        out_ref[v, 0] = jnp.where(hit, value, state_ref[v, 0])


def run_finish(state, cells, values):
    nvar, rows, width_y, width_z = state.shape
    points = cells.shape[0] * cells.shape[1]
    block = pl.BlockSpec((nvar, 1, width_y, width_z), lambda x: (0, x, 0, 0))
    vmem = pl.BlockSpec(memory_space=pltpu.VMEM)
    return pl.pallas_call(
        functools.partial(finish_kernel, width_z.bit_length() - 1),
        grid=(rows,),
        out_shape=jax.ShapeDtypeStruct(state.shape, F32),
        in_specs=[block, vmem, vmem],
        out_specs=block,
        scratch_shapes=[
            pltpu.VMEM((rows * width_y, points), BF16),
            pltpu.VMEM((width_z, points), BF16),
            pltpu.VMEM((2 * nvar, 2 * SUB, points), BF16),
            pltpu.VMEM(((2 * nvar + 1) * width_y, points), BF16),
        ],
        compiler_params=pltpu.CompilerParams(vmem_limit_bytes=VMEM_LIMIT),
        name="finish",
    )(state, cells, values)


def shards(
    state_now, state_prev, viscosity, jacobian, donor_cell, interp_weight, recv_cell, pair_tiles
):
    state, values, cells = run_main(
        jacobian[0], pair_tiles[0], state_now[0], state_prev[0], viscosity[0],
        donor_cell[0, 0], interp_weight[0, 0], recv_cell[0, 0],
    )
    return run_finish(state, cells, values)[None]


def solution(mesh):
    in_specs = (
        P("comp", None, "blk", None, None),
        P("comp", None, "blk", None, None),
        P("comp", "blk", None, None),
        P("comp", None, None, None),
        P("comp", "blk", None, None, None, None),
        P("comp", "blk", None, None, None, None),
        P("comp", "blk", None, None, None),
        P("blk", None, None),
    )
    out_specs = P("comp", None, "blk", None, None)
    return jax.shard_map(shards, mesh=mesh, in_specs=in_specs, out_specs=out_specs, check_vma=False)
```

```python
import functools

import jax
import jax.numpy as jnp
from jax import lax
from jax.experimental import pallas as pl
from jax.experimental.pallas import tpu as pltpu
from jax.sharding import PartitionSpec as P

SUBITERS = 2


time_scale = 0.5
pseudo_diag = 2.5

MESH = pl.DeviceIdType.MESH
VMEM_LIMIT = 60 * 1024 * 1024
F32 = jnp.float32
BF16 = jnp.bfloat16
I32 = jnp.int32
LANES = 128
SUB = 8
PAD = SUB


def split(value):
    high = value.astype(BF16)
    low = (value - high.astype(F32)).astype(BF16)
    return high, low


def flux_tile(src, coef, x, y, kappa, centred):
    nvar, _, halves, _, _ = src.shape
    lane = lax.broadcasted_iota(I32, (SUB, LANES), 1)
    total = [[None] * halves for _ in range(nvar)]
    for w in range(nvar):
        centre = [src[w, x + 1, h, pl.ds(PAD + y, SUB), :] for h in range(halves)]
        fore = [pltpu.roll(c, LANES - 1, 1) for c in centre]
        back = [pltpu.roll(c, 1, 1) for c in centre]
        for h in range(halves):
            next_z = jnp.where(lane == LANES - 1, fore[h + 1] if h + 1 < halves else 0.0, fore[h])
            last_z = jnp.where(lane == 0, back[h - 1] if h > 0 else 0.0, back[h])
            next_x = src[w, x + 2, h, pl.ds(PAD + y, SUB), :]
            last_x = src[w, x, h, pl.ds(PAD + y, SUB), :]
            next_y = src[w, x + 1, h, pl.ds(PAD + y + 1, SUB), :]
            last_y = src[w, x + 1, h, pl.ds(PAD + y - 1, SUB), :]
            beside = (next_x + last_x) + (next_y + last_y) + (next_z + last_z)
            if centred:
                own = kappa[h] * (6.0 * centre[h] - beside)
            else:
                own = -kappa[h] * beside
            total[w][h] = own if total[w][h] is None else total[w][h] + own
            diffs = (next_x - last_x, next_y - last_y, next_z - last_z)
            for v in range(nvar):
                term = None
                for d in range(3):
                    part = coef[(d * nvar + v) * nvar + w] * diffs[d]
                    term = part if term is None else term + part
                total[v][h] = term if total[v][h] is None else total[v][h] + term
    return total


def fill_hots(cells, row_hot, z_hot, shift):
    tiles, tile = cells.shape
    pairs = row_hot.shape[0]
    width_z = z_hot.shape[0]

    def one(t, carry):
        cell = cells[pl.ds(t, 1), :]
        pair = lax.shift_right_arithmetic(cell, shift)
        depth = jnp.bitwise_and(cell, width_z - 1)
        at = pl.ds(pl.multiple_of(t * tile, tile), tile)
        here = lax.broadcasted_iota(I32, (pairs, tile), 0) == pair
        row_hot[:, at] = jnp.where(here, 1.0, 0.0).astype(BF16)
        deep = lax.broadcasted_iota(I32, (width_z, tile), 0) == depth
        z_hot[:, at] = jnp.where(deep, 1.0, 0.0).astype(BF16)
        return carry

    lax.fori_loop(0, tiles, one, 0)


def fill_values(values, spread):
    comps, slots, nvar, tile = values.shape
    depth = spread.shape[1]

    def one(t, carry):
        high, low = split(values[lax.div(t, slots), lax.rem(t, slots)])
        at = pl.ds(pl.multiple_of(t * tile, tile), tile)
        for v in range(nvar):
            spread[v, :, at] = jnp.broadcast_to(high[v : v + 1].astype(F32), (depth, tile)).astype(BF16)
            spread[nvar + v, :, at] = jnp.broadcast_to(low[v : v + 1].astype(F32), (depth, tile)).astype(BF16)
        return carry

    lax.fori_loop(0, comps * slots, one, 0)


def place_planes(planes, width_y, row_hot, z_hot, spread):
    parts, depth, points = spread.shape
    nvar = parts // 2
    chunk = 2 * LANES
    total = None
    for t in range(points // chunk):
        at = pl.ds(t * chunk, chunk)
        blocks = []
        for x in planes:
            rows = row_hot[pl.ds(pl.multiple_of(x * width_y, width_y), width_y), at]
            for j in range(parts):
                blocks.append(rows * jnp.concatenate([spread[j, :, at]] * (width_y // depth), axis=0))
            blocks.append(rows)
        part = lax.dot_general(
            jnp.concatenate(blocks, axis=0), z_hot[:, at], (((1,), (1,)), ((), ())), preferred_element_type=F32
        )
        total = part if total is None else total + part
    results = []
    for i in range(len(planes)):
        rows = [total[(i * (parts + 1) + j) * width_y :][:width_y] for j in range(parts + 1)]
        results.append(([rows[v] + rows[nvar + v] for v in range(nvar)], rows[parts] > 0.5))
    return results


def main_kernel(
    count, comps, jac_ref, live_ref, now_ref, prev_ref, kappa_ref, donor_ref, weight_ref, recv_ref,
    out_ref, arrived, cells,
    state, first, second, rstar, hist, kappa, scale, coef,
    packed, values, held, weight_land, landing, row_hot, z_hot, spread, z_pick, row_weight, inner_part, passing,
    load_sem, halo_send, halo_recv, pass_send, pass_recv, weight_send, weight_recv, value_send, value_recv, save_sem,
):
    me = lax.axis_index("blk")
    mine = lax.axis_index("comp")
    right = lax.rem(me + 1, count)
    left = lax.rem(me + count - 1, count)
    has_left = me > 0
    has_right = me < count - 1
    nvar, rows, halves, width_y, _ = rstar.shape
    width_z = halves * LANES
    shift = width_z.bit_length() - 1
    chunks = width_y // SUB
    slots, corners, tile = donor_ref.shape[1:]
    fields = [state, first, second]
    inside = pl.ds(PAD, width_y)
    edge = rows - 1
    group = 2

    def lanes(h):
        return pl.ds(h * LANES, LANES)

    loads = []
    for h in range(halves):
        for x in (0, edge):
            loads.append((now_ref.at[:, x, :, lanes(h)], state.at[:, x + 1, h, inside, :]))
    for h in range(halves):
        loads.append((now_ref.at[:, pl.ds(1, rows - 2), :, lanes(h)], state.at[:, pl.ds(2, rows - 2), h, inside, :]))
    for h in range(halves):
        loads.append((kappa_ref.at[:, :, lanes(h)], kappa.at[:, h]))
    for h in range(halves):
        loads.append((prev_ref.at[:, :, :, lanes(h)], hist.at[:, :, h]))
    loads = [pltpu.make_async_copy(src, dst, load_sem.at[i]) for i, (src, dst) in enumerate(loads)]
    for load in loads:
        load.start()

    barrier = pltpu.get_barrier_semaphore()

    @pl.when(has_left)
    def _():
        pl.semaphore_signal(barrier, inc=1, device_id={"blk": left}, device_id_type=MESH)

    @pl.when(has_right)
    def _():
        pl.semaphore_signal(barrier, inc=1, device_id={"blk": right}, device_id_type=MESH)

    for d in range(1, comps):
        peer = lax.rem(mine + d, comps)
        pl.semaphore_signal(barrier, inc=1, device_id={"comp": peer}, device_id_type=MESH)

    detour = chunks // 4 if count == 4 else 0
    direct = chunks - detour
    across = lax.rem(me + 2, count)
    if detour:
        pl.semaphore_signal(barrier, inc=1, device_id={"blk": across}, device_id_type=MESH)

    def blank_pads(x, carry):
        for field in fields:
            for v in range(nvar):
                for h in range(halves):
                    field[v, x + 1, h, 0:PAD, :] = jnp.zeros((PAD, LANES), F32)
                    field[v, x + 1, h, PAD + width_y :, :] = jnp.zeros((field.shape[3] - PAD - width_y, LANES), F32)
        return carry

    lax.fori_loop(0, rows, blank_pads, 0)

    def blank_plane(x):
        for field in fields:
            for v in range(nvar):
                for h in range(halves):
                    field[v, x, h, PAD : PAD + width_y, :] = jnp.zeros((width_y, LANES), F32)

    @pl.when(jnp.logical_not(has_left))
    def _():
        blank_plane(0)

    @pl.when(jnp.logical_not(has_right))
    def _():
        blank_plane(rows + 1)

    def to_left(sub, k, c):
        at = pl.ds(PAD + c * SUB, SUB)
        return pltpu.make_async_remote_copy(
            src_ref=fields[k].at[:, 1, :, at, :], dst_ref=fields[k].at[:, rows + 1, :, at, :],
            send_sem=halo_send.at[sub, k, 1, c], recv_sem=halo_recv.at[sub, k, 1, c],
            device_id={"blk": left}, device_id_type=MESH,
        )

    def to_right(sub, k, c):
        at = pl.ds(PAD + c * SUB, SUB)
        return pltpu.make_async_remote_copy(
            src_ref=fields[k].at[:, rows, :, at, :], dst_ref=fields[k].at[:, 0, :, at, :],
            send_sem=halo_send.at[sub, k, 0, c], recv_sem=halo_recv.at[sub, k, 0, c],
            device_id={"blk": right}, device_id_type=MESH,
        )

    def aside(sub, k, c, x, side):
        at = pl.ds(PAD + c * SUB, SUB)
        return pltpu.make_async_remote_copy(
            src_ref=fields[k].at[:, x, :, at, :], dst_ref=passing.at[sub, k, c - direct],
            send_sem=halo_send.at[sub, k, side, c], recv_sem=pass_recv.at[sub, k, c - direct],
            device_id={"blk": across}, device_id_type=MESH,
        )

    def onward(sub, k, c, x, side, target):
        at = pl.ds(PAD + c * SUB, SUB)
        return pltpu.make_async_remote_copy(
            src_ref=passing.at[sub, k, c - direct], dst_ref=fields[k].at[:, x, :, at, :],
            send_sem=pass_send.at[sub, k, c - direct], recv_sem=halo_recv.at[sub, k, side, c],
            device_id={"blk": target}, device_id_type=MESH,
        )

    def start(sub, k, c):
        if c < direct:
            @pl.when(has_left)
            def _():
                to_left(sub, k, c).start()

            @pl.when(has_right)
            def _():
                to_right(sub, k, c).start()
        else:
            @pl.when(jnp.logical_or(me == 1, me == 3))
            def _():
                to_left(sub, k, c).start()

            @pl.when(me == 2)
            def _():
                aside(sub, k, c, 1, 1).start()

            @pl.when(jnp.logical_or(me == 0, me == 2))
            def _():
                to_right(sub, k, c).start()

            @pl.when(me == 1)
            def _():
                aside(sub, k, c, rows, 0).start()

    def forward(sub, k, c):
        if c >= direct:
            @pl.when(me == 3)
            def _():
                aside(sub, k, c, rows, 0).wait_recv()
                onward(sub, k, c, 0, 0, left).start()

            @pl.when(me == 0)
            def _():
                aside(sub, k, c, 1, 1).wait_recv()
                onward(sub, k, c, rows + 1, 1, right).start()

    def forwarded(sub, k):
        for c in range(direct, chunks):
            @pl.when(me == 3)
            def _(c=c):
                onward(sub, k, c, 0, 0, left).wait_send()

            @pl.when(me == 0)
            def _(c=c):
                onward(sub, k, c, rows + 1, 1, right).wait_send()

    def arrive(sub, k, c):
        @pl.when(has_left)
        def _():
            to_right(sub, k, c).wait_recv()

        @pl.when(has_right)
        def _():
            to_left(sub, k, c).wait_recv()

    def sent(sub, k):
        for c in range(chunks):
            @pl.when(has_left)
            def _(c=c):
                to_left(sub, k, c).wait_send()

            @pl.when(has_right)
            def _(c=c):
                to_right(sub, k, c).wait_send()

    def comp_copy(d, source, target, send_sem, recv_sem):
        peer = lax.rem(mine + d, comps)
        return pltpu.make_async_remote_copy(
            src_ref=source.at[peer], dst_ref=target.at[d], send_sem=send_sem, recv_sem=recv_sem,
            device_id={"comp": peer}, device_id_type=MESH,
        )

    def weight_copy(d):
        return comp_copy(d, weight_ref, weight_land, weight_send.at[d], weight_recv.at[d])

    def value_copy(sub, d):
        return comp_copy(d, values.at[sub], landing.at[sub], value_send.at[sub, d], value_recv.at[sub, d])

    def tile_step(k, x, c):
        y = c * SUB
        at = pl.ds(y, SUB)
        own = [kappa[x, h, at, :] for h in range(halves)]
        flow = flux_tile(fields[k], coef, x, y, own, k == 0)
        for h in range(halves):
            factor = scale[x, h, at, :]
            for v in range(nvar):
                centre = fields[0][v, x + 1, h, pl.ds(PAD + y, SUB), :]
                if k == 0:
                    base = (3.0 * time_scale) * centre + hist[v, x, h, at, :] + flow[v][h]
                    rstar[v, x, h, at, :] = base
                    first[v, x + 1, h, pl.ds(PAD + y, SUB), :] = base * factor
                else:
                    step = (rstar[v, x, h, at, :] + flow[v][h]) * factor
                    if k == 1:
                        second[v, x + 1, h, pl.ds(PAD + y, SUB), :] = step
                    else:
                        state[v, x + 1, h, pl.ds(PAD + y, SUB), :] = centre + step

    def planes(k, low, high):
        def one(x, carry):
            for c in range(chunks):
                tile_step(k, x, c)
            return carry

        lax.fori_loop(low, high, one, 0)

    def edges(k, c):
        def one(i, carry):
            tile_step(k, i * edge, c)
            return carry

        lax.fori_loop(0, 2, one, 0)

    def pack(low, high, stride, place):
        def one(i, carry):
            x = low + i * stride
            for v in range(nvar):
                at = pl.ds(pl.multiple_of(((place + i) * nvar + v) * width_y, width_y), width_y)
                for h in range(halves):
                    upper, lower = split(state[v, x + 1, h, inside, :])
                    packed[at, h * LANES : (h + 1) * LANES] = upper
                    packed[at, width_z + h * LANES : width_z + (h + 1) * LANES] = lower
            return carry

        lax.fori_loop(0, high, one, 0)

    def fill_picks(t, carry):
        c, s = lax.div(t, slots), lax.rem(t, slots)
        base = donor_ref[c, s, 0:1, :]
        weights = held[c, s]
        pair = lax.shift_right_logical(base, shift)
        depth = jnp.bitwise_and(base, width_z - 1)
        depth = jnp.concatenate([depth, depth + 1], axis=1)
        pair = jnp.concatenate([pair, pair], axis=1)
        at_z = lax.broadcasted_iota(I32, (width_z, 2 * tile), 0)
        z_pick[t] = jnp.where(at_z == depth, 1.0, 0.0).astype(BF16)
        at_pair = lax.broadcasted_iota(I32, (rows * width_y, 2 * tile), 0) - pair
        spread_row = jnp.zeros((rows * width_y, 2 * tile), F32)
        for a in range(2):
            for b in range(2):
                k = 4 * a + 2 * b
                row = jnp.concatenate([weights[k : k + 1], weights[k + 1 : k + 2]], axis=1)
                spread_row = jnp.where(at_pair == a * width_y + b, row, spread_row)
        row_weight[t] = spread_row
        return carry

    def interpolate(t, where, place):
        size = nvar * width_y
        hot = jnp.concatenate([z_pick[t], z_pick[t]], axis=0)
        found = jnp.dot(packed[place * size : (place + len(where)) * size, :], hot, preferred_element_type=F32)
        total = None
        for i, x in enumerate(where):
            weight = row_weight[t, x * width_y : (x + 1) * width_y, :].reshape(1, chunks, SUB, 2 * tile)
            part = (found[i * size : (i + 1) * size].reshape(nvar, chunks, SUB, 2 * tile) * weight).sum(axis=1)
            total = part if total is None else total + part
        return total

    for load in loads[: 2 * halves]:
        load.wait()
    blocks = has_left.astype(I32) + has_right.astype(I32)
    pl.semaphore_wait(barrier, blocks + comps - 1 + (1 if detour else 0))
    for c in range(chunks):
        start(0, 0, c)
    for d in range(1, comps):
        weight_copy(d).start()
    for d in range(3):
        for v in range(nvar):
            for w in range(nvar):
                coef[(d * nvar + v) * nvar + w] = jnp.full((SUB, LANES), 0.5 * jac_ref[d, v, w], F32)
    for load in loads[2 * halves :]:
        load.wait()

    def prepare(x, carry):
        scale[x] = -1.0 / (pseudo_diag + 6.0 * kappa[x])
        for v in range(nvar):
            hist[v, x] = time_scale * hist[v, x] - (4.0 * time_scale) * state[v, x + 1, :, inside, :]
        return carry

    lax.fori_loop(0, rows, prepare, 0)

    for sub in range(SUBITERS):
        if sub == 0:
            planes(0, 1, edge)
        for c in range(direct, chunks):
            forward(sub, 0, c)
        if sub > 0:
            planes(0, 1, edge)
        if sub == 0:
            for c in range(comps):
                alive = live_ref[c, mine]
                slot = lax.broadcasted_iota(I32, (slots, tile), 0)
                cells[c * slots : (c + 1) * slots, :] = jnp.where(slot < alive, recv_ref[c], -1)
            fill_hots(cells, row_hot, z_hot, shift)
            for d in range(1, comps):
                weight_copy(d).wait()
                held[lax.rem(mine - d + comps, comps)] = weight_land[d]
            held[mine] = weight_ref[mine]
            lax.fori_loop(0, comps * slots, fill_picks, 0)
        for c in range(chunks):
            arrive(sub, 0, c)
            edges(0, c)
            start(sub, 1, c)
        low = 1
        for c in range(chunks):
            if c + direct < chunks:
                forward(sub, 1, c + direct)
            arrive(sub, 1, c)
            edges(1, c)
            start(sub, 2, c)
            high = low + (edge - low + chunks - c - 1) // (chunks - c)
            planes(1, low, high)
            low = high
        half = (edge + 1) // 2
        for c in range(direct, chunks - 1):
            forward(sub, 2, c)
        planes(2, 1, half)
        if detour:
            forward(sub, 2, chunks - 1)
        planes(2, half, edge)
        pack(1, rows - 2, 1, 0)

        def interior(i, carry):
            tiles = [i * group * slots + j for j in range(group * slots)]
            found = [interpolate(t, tuple(range(1, edge)), 0) for t in tiles]
            for t, part in zip(tiles, found):
                inner_part[t] = part
            return carry

        lax.fori_loop(0, comps // group, interior, 0)
        sent(sub, 0)
        for c in range(chunks):
            arrive(sub, 2, c)
            edges(2, c)
        pack(0, 2, edge, rows - 2)

        def boundary(i, carry, sub=sub):
            peers = [lax.rem(mine + i * group + 1 + j, comps) for j in range(group)]
            tiles = [(peer, s) for peer in peers for s in range(slots)]
            found = [interpolate(peer * slots + s, (0, edge), rows - 2) for peer, s in tiles]
            for (peer, s), part in zip(tiles, found):
                total = (part + inner_part[peer * slots + s]).sum(axis=1)
                values[sub, peer, s] = total[:, :tile] + total[:, tile:]

            @pl.when(i > 0)
            def _():
                for j in range(group):
                    value_copy(sub, (i - 1) * group + 1 + j).start()

            return carry

        lax.fori_loop(0, comps // group, boundary, 0)
        for d in range(comps - group + 1, comps):
            value_copy(sub, d).start()
        if sub == SUBITERS - 1:
            saves = [
                pltpu.make_async_copy(
                    state.at[:, pl.ds(1, rows), h, inside, :], out_ref.at[:, :, :, lanes(h)], save_sem.at[h]
                )
                for h in range(halves)
            ]
            for save in saves:
                save.start()
        sent(sub, 1)
        sent(sub, 2)
        for k in range(3):
            forwarded(sub, k)
        arrived[mine] = values[sub, mine]

        def collect(d, carry, sub=sub):
            value_copy(sub, d).wait_recv()
            arrived[lax.rem(mine - d + comps, comps)] = landing[sub, d]
            return carry

        lax.fori_loop(1, comps, collect, 0)
        if sub < SUBITERS - 1:
            fill_values(arrived, spread)

            def place(planes):
                for x, (value, hit) in zip(planes, place_planes(planes, width_y, row_hot, z_hot, spread)):
                    for v in range(nvar):
                        for h in range(halves):
                            side = slice(h * LANES, (h + 1) * LANES)
                            old = state[v, x + 1, h, inside, :]
                            state[v, x + 1, h, inside, :] = jnp.where(hit[:, side], value[v][:, side], old)

            place((0, edge))
            for c in range(chunks):
                start(sub + 1, 0, c)

            def inner(i, carry):
                place((2 * i + 1, 2 * i + 2))
                return carry

            lax.fori_loop(0, (rows - 2) // 2, inner, 0)
    for sub in range(SUBITERS):
        for d in range(1, comps):
            value_copy(sub, d).wait_send()
    for save in saves:
        save.wait()


def run_main(jac, live, now, prev, kappa, donor, weights, recv):
    count = lax.axis_size("blk")
    nvar, rows, width_y, width_z = now.shape
    comps, slots, corners, tile = weights.shape
    halves = width_z // LANES
    chunks = width_y // SUB
    points = comps * slots * tile
    pairs = rows * width_y
    vmem = pl.BlockSpec(memory_space=pltpu.VMEM)
    smem = pl.BlockSpec(memory_space=pltpu.SMEM)
    hbm = pl.BlockSpec(memory_space=pl.ANY)
    field = pltpu.VMEM((nvar, rows + 2, halves, width_y + 2 * PAD, LANES), F32)
    plain = pltpu.VMEM((nvar, rows, halves, width_y, LANES), F32)
    single = pltpu.VMEM((rows, halves, width_y, LANES), F32)
    dma = pltpu.SemaphoreType.DMA
    fringe = (comps, slots, nvar, tile)
    scratch = [
        field, field, field, plain, plain, single, single,
        pltpu.VMEM((3 * nvar * nvar, SUB, LANES), F32),
        pltpu.VMEM((nvar * pairs, 2 * width_z), BF16),
        pltpu.VMEM((SUBITERS,) + fringe, F32),
        pltpu.VMEM(weights.shape, F32),
        pltpu.VMEM(weights.shape, F32),
        pltpu.VMEM((SUBITERS,) + fringe, F32),
        pltpu.VMEM((pairs, points), BF16),
        pltpu.VMEM((width_z, points), BF16),
        pltpu.VMEM((2 * nvar, 2 * SUB, points), BF16),
        pltpu.VMEM((comps * slots, width_z, 2 * tile), BF16),
        pltpu.VMEM((comps * slots, pairs, 2 * tile), F32),
        pltpu.VMEM((comps * slots, nvar, SUB, 2 * tile), F32),
        pltpu.VMEM((SUBITERS, 3, chunks // 2, nvar, halves, SUB, LANES), F32),
        dma((6 * halves,)),
        dma((SUBITERS, 3, 2, chunks)), dma((SUBITERS, 3, 2, chunks)),
        dma((SUBITERS, 3, chunks // 2)), dma((SUBITERS, 3, chunks // 2)),
        dma((comps,)), dma((comps,)),
        dma((SUBITERS, comps)), dma((SUBITERS, comps)),
        dma((halves,)),
    ]
    return pl.pallas_call(
        functools.partial(main_kernel, count, comps),
        out_shape=[
            jax.ShapeDtypeStruct(now.shape, F32),
            jax.ShapeDtypeStruct(fringe, F32),
            jax.ShapeDtypeStruct((comps * slots, tile), I32),
        ],
        in_specs=[smem, smem, hbm, hbm, hbm, vmem, vmem, vmem],
        out_specs=[hbm, vmem, vmem],
        scratch_shapes=scratch,
        compiler_params=pltpu.CompilerParams(
            collective_id=0, has_side_effects=True, vmem_limit_bytes=VMEM_LIMIT
        ),
        name="subiterate",
    )(jac, live, now, prev, kappa, donor, weights, recv)


def finish_kernel(shift, state_ref, cells_ref, value_ref, out_ref, row_hot, z_hot, spread):
    nvar, together, width_y, width_z = state_ref.shape
    step = pl.program_id(0)

    @pl.when(step == 0)
    def _():
        fill_hots(cells_ref, row_hot, z_hot, shift)
        fill_values(value_ref, spread)

    planes = [step * together + i for i in range(together)]
    for i, (value, hit) in enumerate(place_planes(planes, width_y, row_hot, z_hot, spread)):
        for v in range(nvar):
            out_ref[v, i] = jnp.where(hit, value[v], state_ref[v, i])


def run_finish(state, cells, values):
    nvar, rows, width_y, width_z = state.shape
    points = cells.shape[0] * cells.shape[1]
    block = pl.BlockSpec((nvar, 2, width_y, width_z), lambda x: (0, x, 0, 0))
    vmem = pl.BlockSpec(memory_space=pltpu.VMEM)
    return pl.pallas_call(
        functools.partial(finish_kernel, width_z.bit_length() - 1),
        grid=(rows // 2,),
        out_shape=jax.ShapeDtypeStruct(state.shape, F32),
        in_specs=[block, vmem, vmem],
        out_specs=block,
        scratch_shapes=[
            pltpu.VMEM((rows * width_y, points), BF16),
            pltpu.VMEM((width_z, points), BF16),
            pltpu.VMEM((2 * nvar, 2 * SUB, points), BF16),
        ],
        compiler_params=pltpu.CompilerParams(vmem_limit_bytes=VMEM_LIMIT),
        name="finish",
    )(state, cells, values)


def shards(
    state_now, state_prev, viscosity, jacobian, donor_cell, interp_weight, recv_cell, pair_tiles
):
    state, values, cells = run_main(
        jacobian[0], pair_tiles[0], state_now[0], state_prev[0], viscosity[0],
        donor_cell[0, 0], interp_weight[0, 0], recv_cell[0, 0],
    )
    return run_finish(state, cells, values)[None]


def solution(mesh):
    in_specs = (
        P("comp", None, "blk", None, None),
        P("comp", None, "blk", None, None),
        P("comp", "blk", None, None),
        P("comp", None, None, None),
        P("comp", "blk", None, None, None, None),
        P("comp", "blk", None, None, None, None),
        P("comp", "blk", None, None, None),
        P("blk", None, None),
    )
    out_specs = P("comp", None, "blk", None, None)
    return jax.shard_map(shards, mesh=mesh, in_specs=in_specs, out_specs=out_specs, check_vma=False)
```
